32 devices in a mesh: cp: 16 (over z, y, core), tp: 2 (over x).
Axes of the slice: x: 2, y: 2, z: 4, core: 2. Of those that a mesh axis runs over, the one named last changes fastest.
Arguments:
- hidden_in: bfloat16 [4096, 5120], P('cp', 'tp'), may hold values from -6 to 6
- norm_gain: float32 [5120], replicated, may hold values from 0.25 to 1.75
- seq_lengths: int32 [16], replicated, may hold values from 1 to 3072, 4096 in all
- w_query: bfloat16 [5120, 3072], P(None, 'tp'), may hold values from -0.078125 to 0.078125
- b_query: bfloat16 [3072], P('tp'), may hold values from -400 to 400
- w_key: bfloat16 [5120, 1024], P(None, 'tp'), may hold values from -0.078125 to 0.078125
- b_key: bfloat16 [1024], P('tp'), may hold values from -3 to 3
- w_value: bfloat16 [5120, 1024], P(None, 'tp'), may hold values from -0.078125 to 0.078125
- b_value: bfloat16 [1024], P('tp'), may hold values from -3 to 3
- w_out: bfloat16 [3072, 5120], P(None, 'tp'), may hold values from -0.109375 to 0.109375
Outputs:
- mixed: bfloat16 [4096, 5120], P('cp', 'tp')
- k_cache: bfloat16 [4096, 1024], P('cp', 'tp')
- v_cache: bfloat16 [4096, 1024], P('cp', 'tp')
The draws below stay inside these ranges and needn't reach their ends.
Inputs may be any that keep to these rules, and one draw needn't show every extreme that they name: `seq_lengths`: they sum to 4096; the longest is exactly 3072.
All inputs are finite; a program needn't handle non-finite values.
Results may differ from the reference program's by a relative error of at most 0.012.
The reference program's roundings to bfloat16 on the way (of `normed`, `query`, `weights` and `attended`) count: a program that leaves them out, or rounds other values in their place, can miss the bound.
Values may be sent and summed in bfloat16 or wider, within the bound.
No kernel may reach another device: no remote copies, remote signals or barrier semaphores. Data moves between devices by JAX's collectives and lax.ppermute only.
A program may use at most 128 MiB of HBM per device.

```python
import math
import jax
import jax.numpy as jnp
import numpy as np
from jax import lax

D = 5120
KVH = 8
HD = 128
QH = 24
SEQS = 16
TOKENS = 4096
MOST = 3072


def draw_b_query(key, part):
    base = jax.random.normal(jax.random.fold_in(key, 11), (QH * HD,), jnp.float32)
    return jnp.clip(0.5 * base, -3.0, 3.0).astype(jnp.bfloat16)


def shard_levels(own_key, extent, shards, least, top_value):
    def one(axis_at, blocks):
        steps = jax.random.uniform(jax.random.fold_in(jax.random.fold_in(own_key, 6), axis_at), (blocks,), jnp.float32, least / len(shards), top_value / len(shards))
        return jnp.repeat(jnp.exp(steps), extent[axis_at] // blocks).reshape((-1,) + (1,) * (len(extent) - axis_at - 1))

    level = one(*shards[0])
    for cut in shards[1:]:
        level = level * one(*cut)
    return level


def length_profile(number_of, total, limit, skew):
    portions = [(1 << 20) // math.isqrt(grade ** skew) + 1 for grade in range(2, number_of + 1)]
    spare, holding = total - limit - (number_of - 1), [1] * (number_of - 1)
    while spare > 0:
        candidates = [i for i in range(number_of - 1) if holding[i] < limit]
        whole, remaining = sum([portions[i] for i in candidates]), spare
        for i in candidates:
            more = min(limit - holding[i], max(1, remaining * portions[i] // whole), spare)
            holding[i] = holding[i] + more
            spare = spare - more
    return np.array([limit] + holding)


def ragged_sizes(rng, number_of, total, bound, slope):
    if number_of == 2:
        one = jax.random.randint(rng, (), max(1, total - bound), min(bound, total - 1) + 1)
        return jnp.stack([one, total - one])
    lengths = jnp.asarray(length_profile(number_of, total, bound, slope), jnp.int32)
    twos = (number_of - 1) // 2
    donor, sink = lengths[1:1 + 2 * twos:2], lengths[2:2 + 2 * twos:2]
    margin = jnp.minimum(donor - 1, bound - sink)
    shifted = jax.random.randint(jax.random.fold_in(rng, 1), (twos,), 0, 1 << 20) % (margin + 1)
    lengths = lengths.at[1:1 + 2 * twos:2].set(donor - shifted).at[2:2 + 2 * twos:2].set(sink + shifted)
    return lengths[jax.random.permutation(jax.random.fold_in(rng, 2), number_of)]


def gaussian(rng, dims, scale, reach, shards=(), kind=jnp.bfloat16):
    values = scale * jax.random.normal(rng, dims, jnp.float32)
    if shards:
        values = values * shard_levels(rng, dims, shards, -0.22, 0.18)
    return jnp.clip(values, -reach, reach).astype(kind)


def setup_inputs(seed: int = 0) -> dict:
    streams_of = jax.random.split(jax.random.key(seed), 11)
    return {
        "hidden_in": gaussian(streams_of[0], (TOKENS, D), 1.0, 6.0, ((0, 16), (1, 2))),
        "norm_gain": jnp.clip(1.0 + 0.15 * jax.random.normal(streams_of[1], (D,), jnp.float32), 0.25, 1.75),
        "seq_lengths": ragged_sizes(streams_of[2], SEQS, TOKENS, MOST, 2).astype(jnp.int32),
        "w_query": gaussian(streams_of[3], (D, QH * HD), D ** -0.5, 0.078125, ((1, 2),)),
        "b_query": draw_b_query(jax.random.fold_in(streams_of[10], 71), 0),
        "w_key": gaussian(streams_of[5], (D, KVH * HD), D ** -0.5, 0.078125, ((1, 2),)),
        "b_key": gaussian(streams_of[6], (KVH * HD,), 0.5, 3.0, ((0, 2),)),
        "w_value": gaussian(streams_of[7], (D, KVH * HD), D ** -0.5, 0.078125, ((1, 2),)),
        "b_value": gaussian(streams_of[8], (KVH * HD,), 0.5, 3.0, ((0, 2),)),
        "w_out": gaussian(streams_of[9], (QH * HD, D), (QH * HD) ** -0.5, 0.109375, ((1, 2),)),
    }


EPS = 1e-06
ROPE_BASE = 1000000.0
NEG = -1e+30

def doc_tables(seq_lengths, positions):
    ends = jnp.cumsum(seq_lengths).astype(jnp.int32)
    starts = (ends - seq_lengths).astype(jnp.int32)
    after = positions[:, None] >= ends[None, :]
    docs = lax.optimization_barrier(jnp.sum(after.astype(jnp.int32), axis=1)).astype(jnp.int32)
    inside = (positions[:, None] >= starts[None, :]) & jnp.logical_not(after)
    offset = lax.optimization_barrier(jnp.sum(jnp.where(inside, starts[None, :], 0), axis=1)).astype(jnp.int32)
    return (docs, (positions - offset).astype(jnp.int32))

def rotate(values, positions):
    half = values.shape[-1] // 2
    freq = ROPE_BASE ** (-jnp.arange(half, dtype=jnp.float32) / half)
    angle = positions.astype(jnp.float32)[:, None] * freq[None, :]
    cosine = jnp.cos(angle)[:, None, :]
    sine = jnp.sin(angle)[:, None, :]
    first = values[..., :half]
    second = values[..., half:]
    return jnp.concatenate([first * cosine - second * sine, second * cosine + first * sine], axis=-1)

def reference(hidden_in, norm_gain, seq_lengths, w_query, b_query, w_key, b_key, w_value, b_value, w_out):
    positions = jnp.arange(TOKENS, dtype=jnp.int32)
    docs, local_pos = doc_tables(seq_lengths, positions)
    widened = hidden_in.astype(jnp.float32)
    normed = (widened * lax.rsqrt(lax.optimization_barrier(jnp.mean(widened * widened, axis=-1, keepdims=True)) + EPS) * norm_gain).astype(jnp.bfloat16)
    query = jnp.dot(normed, w_query, preferred_element_type=jnp.float32) + b_query.astype(jnp.float32)
    query = rotate(query.reshape(TOKENS, QH, HD), local_pos).astype(jnp.bfloat16)
    keys = jnp.dot(normed, w_key, preferred_element_type=jnp.float32) + b_key.astype(jnp.float32)
    keys = rotate(keys.reshape(TOKENS, KVH, HD), local_pos).astype(jnp.bfloat16)
    values = (jnp.dot(normed, w_value, preferred_element_type=jnp.float32) + b_value.astype(jnp.float32)).astype(jnp.bfloat16)
    value_heads = values.reshape(TOKENS, KVH, HD)
    group = QH // KVH
    grouped = query.reshape(TOKENS, KVH, group, HD)
    block = math.gcd(512, TOKENS)
    window = min(TOKENS, MOST + block)
    scale = HD ** (-0.5)

    def one_block(index):
        q_start = (index * block).astype(jnp.int32)
        k_start = jnp.clip(q_start - MOST, 0, TOKENS - window).astype(jnp.int32)
        q_rows = lax.dynamic_slice_in_dim(grouped, q_start, block, 0).astype(jnp.float32)
        k_rows = lax.dynamic_slice_in_dim(keys, k_start, window, 0).astype(jnp.float32)
        v_rows = lax.dynamic_slice_in_dim(value_heads, k_start, window, 0).astype(jnp.float32)
        q_pos = q_start + jnp.arange(block, dtype=jnp.int32)
        k_pos = k_start + jnp.arange(window, dtype=jnp.int32)
        q_doc = lax.dynamic_slice_in_dim(docs, q_start, block, 0)
        k_doc = lax.dynamic_slice_in_dim(docs, k_start, window, 0)
        allowed = (k_pos[None, :] <= q_pos[:, None]) & (k_doc[None, :] == q_doc[:, None])
        scores = jnp.einsum('qhgd,khd->hgqk', q_rows, k_rows) * scale
        highest = lax.optimization_barrier(jnp.max(jnp.where(allowed, scores, NEG), axis=-1, keepdims=True))
        weights = jnp.exp(jnp.where(allowed, scores - highest, NEG))
        totals = lax.optimization_barrier(jnp.sum(weights, axis=-1))
        rounded = lax.optimization_barrier(weights.astype(jnp.bfloat16))
        summed = jnp.einsum('hgqk,khd->qhgd', rounded.astype(jnp.float32), v_rows)
        result = summed / jnp.transpose(totals, (2, 0, 1))[..., None]
        return result.astype(jnp.bfloat16).reshape(block, QH * HD)
    attended = lax.map(one_block, jnp.arange(TOKENS // block, dtype=jnp.int32)).reshape(TOKENS, QH * HD)
    projected = jnp.dot(attended, w_out, preferred_element_type=jnp.float32)
    mixed = (widened + projected).astype(jnp.bfloat16)
    return (mixed, keys.reshape(TOKENS, KVH * HD), values)
```

```python
import functools
import math

import jax
import jax.numpy as jnp
from jax import lax
from jax.experimental import pallas as pl
from jax.experimental.pallas import tpu as pltpu
from jax.sharding import PartitionSpec as P

HD = 128
EPS = 1e-06
ROPE_BASE = 1000000.0
NEG = -1e30
CHUNKS = 2
SIZES = ("cp", "tp")


def doc_tables(seq_lengths, positions):
    ends = jnp.cumsum(seq_lengths)
    starts = ends - seq_lengths
    after = positions[:, None] >= ends[None, :]
    docs = jnp.sum(after.astype(jnp.int32), axis=1)
    inside = (positions[:, None] >= starts[None, :]) & jnp.logical_not(after)
    offset = jnp.sum(jnp.where(inside, starts[None, :], 0), axis=1)
    return (docs, positions - offset)


def rotate(values, positions):
    half = values.shape[-1] // 2
    freq = ROPE_BASE ** (-jnp.arange(half, dtype=jnp.float32) / half)
    angle = positions.astype(jnp.float32)[:, None] * freq[None, :]
    cosine = jnp.cos(angle)[:, None, :]
    sine = jnp.sin(angle)[:, None, :]
    first = values[..., :half]
    second = values[..., half:]
    return jnp.concatenate(
        [first * cosine - second * sine, second * cosine + first * sine], axis=-1
    )


def general(
    hidden_in, norm_gain, seq_lengths, w_query, b_query, w_key, b_key, w_value, b_value, w_out
):
    tok_rows = hidden_in.shape[0]
    gathered = lax.all_gather(hidden_in, "tp", axis=1, tiled=True)
    widened = gathered.astype(jnp.float32)
    normed = (
        widened * lax.rsqrt(jnp.mean(widened * widened, axis=-1, keepdims=True) + EPS) * norm_gain
    ).astype(jnp.bfloat16)
    cp_index = lax.axis_index("cp")
    positions = cp_index * tok_rows + jnp.arange(tok_rows, dtype=jnp.int32)
    docs, local_pos = doc_tables(seq_lengths, positions)
    query = jnp.dot(normed, w_query, preferred_element_type=jnp.float32) + b_query.astype(
        jnp.float32
    )
    query = rotate(query.reshape(tok_rows, -1, HD), local_pos).astype(jnp.bfloat16)
    key_heads = jnp.dot(normed, w_key, preferred_element_type=jnp.float32) + b_key.astype(
        jnp.float32
    )
    key_heads = rotate(key_heads.reshape(tok_rows, -1, HD), local_pos).astype(jnp.bfloat16)
    value_flat = (
        jnp.dot(normed, w_value, preferred_element_type=jnp.float32) + b_value.astype(jnp.float32)
    ).astype(jnp.bfloat16)
    kv_heads = key_heads.shape[1]
    value_heads = value_flat.reshape(tok_rows, kv_heads, HD)
    group = query.shape[1] // kv_heads
    grouped = query.reshape(tok_rows, kv_heads, group, HD)
    scale = HD ** (-0.5)

    def update(carried, key_block, value_block, start):
        count = key_block.shape[0]
        key_pos = start + jnp.arange(count, dtype=jnp.int32)
        key_docs, unused_pos = doc_tables(seq_lengths, key_pos)
        allowed = (key_pos[None, :] <= positions[:, None]) & (key_docs[None, :] == docs[:, None])

        def compute(state):
            running, totals, accum = state
            scores = (
                jnp.einsum("qhgd,khd->hgqk", grouped, key_block, preferred_element_type=jnp.float32)
                * scale
            )
            highest = jnp.max(jnp.where(allowed, scores, NEG), axis=-1)
            fresh = jnp.maximum(running, highest)
            weights = jnp.where(allowed, jnp.exp(scores - fresh[..., None]), 0.0)
            factor = jnp.exp(running - fresh)
            totals = totals * factor + jnp.sum(weights, axis=-1)
            added = jnp.einsum(
                "hgqk,khd->qhgd",
                weights.astype(jnp.bfloat16),
                value_block,
                preferred_element_type=jnp.float32,
            )
            accum = accum * jnp.transpose(factor, (2, 0, 1))[..., None] + added
            return (fresh, totals, accum)

        return lax.cond(jnp.any(allowed), compute, lambda state: state, carried)

    carried = (
        jnp.full((kv_heads, group, tok_rows), NEG, jnp.float32),
        jnp.zeros((kv_heads, group, tok_rows), jnp.float32),
        jnp.zeros((tok_rows, kv_heads, group, HD), jnp.float32),
    )
    key_rows = lax.all_gather(key_heads, "cp", axis=0, tiled=True)
    count = key_rows.shape[0]
    width = math.gcd(512, count)
    blocks = count // width
    key_split = key_rows.reshape(blocks, width, kv_heads, HD)
    value_split = lax.all_gather(value_heads, "cp", axis=0, tiled=True).reshape(
        blocks, width, kv_heads, HD
    )

    def advance(state, items):
        return (update(state, items[0], items[1], items[2] * width), None)

    carried, unused_out = lax.scan(
        advance, carried, (key_split, value_split, jnp.arange(blocks, dtype=jnp.int32))
    )
    running, totals, accum = carried
    attended = (
        (accum / jnp.transpose(totals, (2, 0, 1))[..., None])
        .astype(jnp.bfloat16)
        .reshape(tok_rows, -1)
    )
    summed = jnp.dot(
        lax.all_gather(attended, "tp", axis=1, tiled=True),
        w_out,
        preferred_element_type=jnp.float32,
    )
    mixed = (hidden_in.astype(jnp.float32) + summed).astype(jnp.bfloat16)
    return (mixed, key_heads.reshape(tok_rows, -1), value_flat)


def turned(u, cosf, sinf):
    return u * cosf + pltpu.roll(u, HD // 2, 1) * sinf


def kv_kernel(s_ref, own_ref, got_ref, gain_ref, cos_ref, sin_ref, wk_ref, wv_ref, bk_ref, bv_ref,
              k_ref, v_ref, keep_ref, send_ref, normed_ref):
    tp = s_ref[0]
    half = own_ref.shape[1]
    j = pl.program_id(0)

    @pl.when(j == 0)
    def _():
        own = own_ref[...].astype(jnp.float32)
        got = got_ref[...].astype(jnp.float32)
        total = jnp.sum(own * own, axis=1, keepdims=True) + jnp.sum(got * got, axis=1, keepdims=True)
        factor = lax.rsqrt(total / (2 * half) + EPS)
        here = pl.ds(pl.multiple_of(tp * half, half), half)
        there = pl.ds(pl.multiple_of((1 - tp) * half, half), half)
        normed_ref[:, here] = (own * factor * gain_ref[:, here]).astype(jnp.bfloat16)
        normed_ref[:, there] = (got * factor * gain_ref[:, there]).astype(jnp.bfloat16)

    x = normed_ref[...]
    keys = jnp.dot(x, wk_ref[...], preferred_element_type=jnp.float32) + bk_ref[...]
    cosf, sinf = cos_ref[...], sin_ref[...]
    width = keys.shape[1]
    keys = jnp.concatenate(
        [turned(keys[:, i:i + HD], cosf, sinf) for i in range(0, width, HD)], axis=1
    ).astype(jnp.bfloat16)
    values = (jnp.dot(x, wv_ref[...], preferred_element_type=jnp.float32) + bv_ref[...]).astype(
        jnp.bfloat16
    )
    k_ref[...] = keys
    v_ref[...] = values

    @pl.when(j == 0)
    def _():
        keep_ref[:, :width] = keys
        keep_ref[:, width:] = values

    @pl.when(j == 1)
    def _():
        send_ref[:, :width] = keys
        send_ref[:, width:] = values


def project_kv(scalars, own, got, gain, cosf, sinf, wk, wv, bk, bv):
    rows, half = own.shape
    depth, cols = wk.shape
    width = cols // 2
    whole = lambda shape: pl.BlockSpec(shape, lambda j, s: (0, 0))
    side = lambda j, s: (0, lax.rem(j + s[1], 2))
    bf = jnp.bfloat16
    return pl.pallas_call(
        kv_kernel,
        out_shape=(
            jax.ShapeDtypeStruct((rows, cols), bf),
            jax.ShapeDtypeStruct((rows, cols), bf),
            jax.ShapeDtypeStruct((rows, cols), bf),
            jax.ShapeDtypeStruct((rows, cols), bf),
            jax.ShapeDtypeStruct((rows, depth), bf),
        ),
        grid_spec=pltpu.PrefetchScalarGridSpec(
            num_scalar_prefetch=1,
            grid=(2,),
            in_specs=[
                whole((rows, half)), whole((rows, half)), whole((1, depth)),
                whole((rows, HD)), whole((rows, HD)),
                pl.BlockSpec((depth, width), side), pl.BlockSpec((depth, width), side),
                pl.BlockSpec((1, width), side), pl.BlockSpec((1, width), side),
            ],
            out_specs=[
                pl.BlockSpec((rows, width), side), pl.BlockSpec((rows, width), side),
                whole((rows, cols)), whole((rows, cols)), whole((rows, depth)),
            ],
        ),
        cost_estimate=pl.CostEstimate(
            flops=4 * rows * depth * cols, transcendentals=0, bytes_accessed=4 * depth * cols
        ),
        name="project_kv",
    )(scalars, own, got, gain, cosf, sinf, wk, wv, bk, bv)


def q_kernel(steps, s_ref, *refs):
    x_refs = refs[:CHUNKS]
    cos_ref, sin_ref, w_ref, b_ref, keep_ref, send_ref = refs[CHUNKS:]
    j = pl.program_id(0)
    rows = x_refs[0].shape[0]
    outs = []
    for t, x_ref in enumerate(x_refs):
        q = jnp.dot(x_ref[...], w_ref[...], preferred_element_type=jnp.float32) + b_ref[...]
        cosf = cos_ref[t * rows:(t + 1) * rows, :]
        sinf = sin_ref[t * rows:(t + 1) * rows, :]
        outs.append(jnp.concatenate(
            [turned(q[:, i:i + HD], cosf, sinf) for i in range(0, q.shape[1], HD)], axis=1
        ).astype(jnp.bfloat16))

    @pl.when(j < steps)
    def _():
        for t, out in enumerate(outs):
            keep_ref[t * rows:(t + 1) * rows, :] = out

    @pl.when(j >= steps)
    def _():
        for t, out in enumerate(outs):
            send_ref[t * rows:(t + 1) * rows, :] = out


def project_q(scalars, normed, cosf, sinf, wq, bq):
    rows, depth = normed[0].shape
    tokens = rows * len(normed)
    cols = wq.shape[1]
    width = math.gcd(cols // 2, 2 * HD)
    steps = cols // 2 // width
    whole = lambda shape: pl.BlockSpec(shape, lambda j, s: (0, 0))
    side = lambda j, s: (0, lax.rem(j // steps + s[1], 2) * steps + lax.rem(j, steps))
    return pl.pallas_call(
        functools.partial(q_kernel, steps),
        out_shape=(jax.ShapeDtypeStruct((tokens, cols // 2), jnp.bfloat16),) * 2,
        grid_spec=pltpu.PrefetchScalarGridSpec(
            num_scalar_prefetch=1,
            grid=(2 * steps,),
            in_specs=[whole((rows, depth))] * len(normed) + [
                whole((tokens, HD)), whole((tokens, HD)),
                pl.BlockSpec((depth, width), side), pl.BlockSpec((1, width), side),
            ],
            out_specs=[
                pl.BlockSpec((tokens, width), lambda j, s: (0, jnp.minimum(j, steps - 1))),
                pl.BlockSpec((tokens, width), lambda j, s: (0, jnp.maximum(j - steps, 0))),
            ],
        ),
        cost_estimate=pl.CostEstimate(
            flops=2 * tokens * depth * cols, transcendentals=0, bytes_accessed=2 * depth * cols
        ),
        name="project_q",
    )(scalars, *normed, cosf, sinf, wq, bq)


def attend_kernel(units, heads, group, first, last, t_ref, *refs):
    q_refs, refs = refs[:2], refs[2:]
    pos_ref, low_ref, refs = refs[0], refs[1], refs[2:]
    u_refs, refs = refs[:units], refs[units:]
    if not first:
        (m_in, l_in, acc_in), refs = refs[:3], refs[3:]
    if last:
        out_refs, refs = refs[:2], refs[2:]
        m_ref, l_ref, acc_ref, kv, q_all = refs
    else:
        m_ref, l_ref, acc_ref, kv, q_all = refs
    keys = u_refs[0].shape[0]
    rows = q_refs[0].shape[0]
    tiles = 2 * heads * group
    if first:
        m_ref[...] = jnp.full(m_ref.shape, NEG, jnp.float32)
        l_ref[...] = jnp.zeros(l_ref.shape, jnp.float32)
        acc_ref[...] = jnp.zeros(acc_ref.shape, jnp.float32)
    else:
        m_ref[...] = m_in[...]
        l_ref[...] = l_in[...]
        acc_ref[...] = acc_in[...]
    for n in range(units):
        kv[n] = u_refs[n][...]
    for half in range(2):
        for g in range(heads * group):
            q_all[half * heads * group + g] = q_refs[half][:, g * HD:(g + 1) * HD]
    factor = HD ** (-0.5) * math.log2(math.e)

    def step(n, masked):
        def tile(i, carry):
            half = i // (heads * group)
            head = lax.rem(i, heads * group) // group
            k = kv[n, :, pl.ds(pl.multiple_of(head * HD, HD), HD)]
            v = kv[n, :, pl.ds(pl.multiple_of((heads + head) * HD, HD), HD)]
            s = lax.dot_general(
                k, q_all[i], (((1,), (1,)), ((), ())), preferred_element_type=jnp.float32
            )
            old = m_ref[i]
            if masked:
                at = lax.broadcasted_iota(jnp.int32, (keys, 1), 0)
                at = at + jnp.where(at < keys // 2, t_ref[n, 1], t_ref[n, 2] - keys // 2)
                allowed = (at >= low_ref[half]) & (at <= pos_ref[half])
                s = jnp.where(allowed, s, NEG)
            new = jnp.maximum(old, jnp.max(s, axis=0, keepdims=True))
            p = jnp.exp2((s - new) * factor)
            if masked:
                p = jnp.where(allowed, p, 0.0)
            alpha = jnp.exp2((old - new) * factor)
            m_ref[i] = new
            l_ref[i] = l_ref[i] * alpha + jnp.sum(p, axis=0, keepdims=True)
            added = lax.dot_general(
                v, p.astype(jnp.bfloat16), (((0,), (0,)), ((), ())),
                preferred_element_type=jnp.float32,
            )
            acc_ref[i] = acc_ref[i] * alpha + added
            return carry

        lax.fori_loop(0, tiles, tile, 0)

    def unit(n, carry):
        state = t_ref[n, 0]

        @pl.when(state == 1)
        def _():
            step(n, False)

        @pl.when(state == 2)
        def _():
            step(n, True)

        return carry

    lax.fori_loop(0, units, unit, 0)
    if last:
        for half in range(2):
            for g in range(heads * group):
                i = half * heads * group + g
                out_refs[half][:, g * HD:(g + 1) * HD] = (acc_ref[i] / l_ref[i]).T.astype(
                    jnp.bfloat16
                )


def attend(table, queries, pos, low, units, state, heads, group, last, name):
    rows, cols = queries[0].shape
    keys = units[0].shape[0]
    tiles = 2 * heads * group
    first = state is None
    vm = pl.BlockSpec(memory_space=pltpu.VMEM)
    stat = jax.ShapeDtypeStruct((tiles, 1, rows), jnp.float32)
    accs = jax.ShapeDtypeStruct((tiles, HD, rows), jnp.float32)
    scratch = [
        pltpu.VMEM((len(units), keys, units[0].shape[1]), jnp.bfloat16),
        pltpu.VMEM((tiles, rows, HD), jnp.bfloat16),
    ]
    if last:
        out_shape = (jax.ShapeDtypeStruct((rows, cols), jnp.bfloat16),) * 2
        scratch = [
            pltpu.VMEM(stat.shape, jnp.float32), pltpu.VMEM(stat.shape, jnp.float32),
            pltpu.VMEM(accs.shape, jnp.float32),
        ] + scratch
    else:
        out_shape = (stat, stat, accs)
    args = [*queries, pos, low, *units] + ([] if first else list(state))
    return pl.pallas_call(
        functools.partial(attend_kernel, len(units), heads, group, first, last),
        out_shape=out_shape,
        in_specs=[pl.BlockSpec(memory_space=pltpu.SMEM)] + [vm] * len(args),
        out_specs=[vm] * len(out_shape),
        scratch_shapes=scratch,
        cost_estimate=pl.CostEstimate(
            flops=4 * tiles * rows * keys * HD * len(units),
            transcendentals=tiles * rows * keys * len(units),
            bytes_accessed=4 * tiles * rows * HD,
        ),
        name=name,
    )(table, *args)


def out_kernel(s_ref, h_ref, *refs):
    a_refs, (w_ref, out_ref) = refs[:4], refs[4:]
    depth = a_refs[0].shape[1]
    total = h_ref[...].astype(jnp.float32)
    for n, a_ref in enumerate(a_refs):
        rows = pl.ds(pl.multiple_of(s_ref[2 + n] * depth, depth), depth)
        total = total + jnp.dot(a_ref[...], w_ref[rows, :], preferred_element_type=jnp.float32)
    out_ref[...] = total.astype(out_ref.dtype)


def project_out(scalars, hidden, pieces, w_out):
    rows, cols = hidden.shape
    depth = w_out.shape[0]
    width = math.gcd(cols, 512)
    whole = lambda a: pl.BlockSpec(a.shape, lambda j, s: (0, 0))
    return pl.pallas_call(
        out_kernel,
        out_shape=jax.ShapeDtypeStruct((rows, cols), jnp.bfloat16),
        grid_spec=pltpu.PrefetchScalarGridSpec(
            num_scalar_prefetch=1,
            grid=(cols // width,),
            in_specs=[pl.BlockSpec((rows, width), lambda j, s: (0, j))]
            + [whole(a) for a in pieces]
            + [pl.BlockSpec((depth, width), lambda j, s: (0, j))],
            out_specs=pl.BlockSpec((rows, width), lambda j, s: (0, j)),
        ),
        cost_estimate=pl.CostEstimate(
            flops=2 * rows * depth * cols, transcendentals=0, bytes_accessed=2 * depth * cols
        ),
        name="project_out",
    )(scalars, hidden, *pieces, w_out)


def local(
    planes, hidden_in, norm_gain, seq_lengths, w_query, b_query, w_key, b_key, w_value, b_value,
    w_out,
):
    rows, half = hidden_in.shape
    part = rows // CHUNKS
    heads = w_key.shape[1] // HD // 2
    group = w_query.shape[1] // w_key.shape[1]
    tp = lax.axis_index("tp")
    cp = lax.axis_index("cp")
    core, row, plane = cp % 2, cp // 2 % 2, cp // 4
    chip = cp // 2
    f32 = jnp.float32

    def pairs(move):
        found = []
        for z in range(planes):
            for y in range(2):
                for c in range(2):
                    for x in range(2):
                        to = move(z, y, c, x)
                        if to is not None:
                            found.append((
                                ((z * 2 + y) * 2 + c) * 2 + x,
                                ((to[0] * 2 + to[1]) * 2 + to[2]) * 2 + to[3],
                            ))
        return found

    over_x = pairs(lambda z, y, c, x: (z, y, c, 1 - x))
    over_c = pairs(lambda z, y, c, x: (z, y, 1 - c, x))
    over_xc = pairs(lambda z, y, c, x: (z, y, 1 - c, 1 - x))

    def up(k):
        return pairs(lambda z, y, c, x: (z + 1, y, c, x) if k <= z + 1 < planes else None)

    def across(k):
        return pairs(
            lambda z, y, c, x: (z, 1 - y, c, x) if z >= k and (k > 0 or y == 0) else None
        )

    def send(a, route):
        return lax.ppermute(a, SIZES, route)

    chunks = [hidden_in[t * part:(t + 1) * part] for t in range(CHUNKS)]
    got = [send(a, over_x) for a in chunks]

    ends = jnp.cumsum(seq_lengths)
    starts = ends - seq_lengths
    chip_pos = jnp.stack([
        cp * rows + jnp.arange(rows, dtype=jnp.int32),
        (cp + 1 - 2 * core) * rows + jnp.arange(rows, dtype=jnp.int32),
    ])
    low = jnp.max(
        jnp.where(starts[None, None, :] <= chip_pos[..., None], starts[None, None, :], 0), axis=-1
    )
    local_pos = (chip_pos - low)[0]
    freq = ROPE_BASE ** (-jnp.arange(HD // 2, dtype=f32) / (HD // 2))
    angle = local_pos.astype(f32)[:, None] * freq[None, :]
    cosine, sine = jnp.cos(angle), jnp.sin(angle)
    cosf = jnp.concatenate([cosine, cosine], axis=1)
    sinf = jnp.concatenate([-sine, sine], axis=1)
    other = (1 - tp) * 2
    scalars = jnp.stack(
        [tp, core, tp * 2 + core, tp * 2 + 1 - core, other + core, other + 1 - core]
    ).astype(jnp.int32)

    span = 2 * rows
    q_from, q_to = chip * span, chip * span + span - 1
    low_min = jnp.min(low)
    low_max = jnp.max(low)
    shift = jnp.array([[k, flip, t] for k in range(planes) for flip in range(2)
                       for t in range(CHUNKS)], jnp.int32)
    source = (plane - shift[:, 0]) * 2 + jnp.where(shift[:, 1] == 0, row, 1 - row)
    first_pos = source * span + core * rows + shift[:, 2] * part
    second_pos = source * span + (1 - core) * rows + shift[:, 2] * part
    k_from = jnp.minimum(first_pos, second_pos)
    k_to = jnp.maximum(first_pos, second_pos) + part - 1
    valid = (plane >= shift[:, 0]) & (k_to >= low_min) & (k_from <= q_to)
    free = (k_from >= low_max) & (k_to <= q_from)
    states = jnp.where(valid, jnp.where(free, 1, 2), 0)
    table = jnp.stack([states, first_pos, second_pos], axis=1).astype(jnp.int32)

    gain = norm_gain[None, :]
    bk, bv, bq = (b.astype(f32)[None, :] for b in (b_key, b_value, b_query))
    k_parts, v_parts, normed, units = [], [], [], [[None] * CHUNKS for _ in range(2 * planes)]
    for t in range(CHUNKS):
        here = slice(t * part, (t + 1) * part)
        k, v, keep, give, norm = project_kv(
            scalars, chunks[t], got[t], gain, cosf[here], sinf[here],
            w_key, w_value, bk, bv,
        )
        k_parts.append(k)
        v_parts.append(v)
        normed.append(norm)
        column = jnp.concatenate([keep, send(give, over_c)], axis=0)
        for k in range(planes):
            units[2 * k][t] = column
            units[2 * k + 1][t] = send(column, across(k))
            if k + 1 < planes:
                column = send(column, up(k + 1))
    q_keep, q_give = project_q(scalars, normed, cosf, sinf, w_query, bq)
    queries = (q_keep, send(q_give, over_c))

    pos, low = chip_pos[:, None, :], low[:, None, :]
    state = None
    for n, planes_here in enumerate(((0,), tuple(range(1, planes - 1)), (planes - 1,))):
        if not planes_here:
            continue
        mine, lines = [], []
        for k in planes_here:
            for flip in range(2):
                for t in range(CHUNKS):
                    mine.append(units[2 * k + flip][t])
                    lines.append((2 * k + flip) * CHUNKS + t)
        state = attend(
            table[lines[0]:lines[-1] + 1], queries, pos, low, mine, state, heads, group,
            planes_here[-1] == planes - 1, f"attend_{n}",
        )
    att_own, att_partner = state
    pieces = (att_own, send(att_partner, over_c), send(att_own, over_x), send(att_partner, over_xc))
    mixed = project_out(scalars, hidden_in, pieces, w_out)
    return (mixed, jnp.concatenate(k_parts, axis=0), jnp.concatenate(v_parts, axis=0))


def solution(mesh):
    placed = (
        P("cp", "tp"),
        P(),
        P(),
        P(None, "tp"),
        P("tp"),
        P(None, "tp"),
        P("tp"),
        P(None, "tp"),
        P("tp"),
        P(None, "tp"),
    )
    out = (P("cp", "tp"), P("cp", "tp"), P("cp", "tp"))

    def call(*args):
        cp, tp = mesh.shape["cp"], mesh.shape["tp"]
        rows = args[0].shape[0] // cp
        kv_heads = args[5].shape[1] // tp // HD
        fits = tp == 2 and cp % 4 == 0 and cp >= 8 and kv_heads % 2 == 0 and rows % 32 == 0
        body = functools.partial(local, cp // 4) if fits else general
        return jax.shard_map(
            body, mesh=mesh, in_specs=placed, out_specs=out, check_vma=False
        )(*args)

    return call
```

```python
import functools
import math

import jax
import jax.numpy as jnp
from jax import lax
from jax.experimental import pallas as pl
from jax.experimental.pallas import tpu as pltpu
from jax.sharding import PartitionSpec as P


HD = 128
EPS = 1e-06
ROPE_BASE = 1000000.0
NEG = -1e30
CHUNKS = 2
SIZES = ("cp", "tp")


def doc_tables(seq_lengths, positions):
    ends = jnp.cumsum(seq_lengths)
    starts = ends - seq_lengths
    after = positions[:, None] >= ends[None, :]
    docs = jnp.sum(after.astype(jnp.int32), axis=1)
    inside = (positions[:, None] >= starts[None, :]) & jnp.logical_not(after)
    offset = jnp.sum(jnp.where(inside, starts[None, :], 0), axis=1)
    return (docs, positions - offset)


def rotate(values, positions):
    half = values.shape[-1] // 2
    freq = ROPE_BASE ** (-jnp.arange(half, dtype=jnp.float32) / half)
    angle = positions.astype(jnp.float32)[:, None] * freq[None, :]
    cosine = jnp.cos(angle)[:, None, :]
    sine = jnp.sin(angle)[:, None, :]
    first = values[..., :half]
    second = values[..., half:]
    return jnp.concatenate(
        [first * cosine - second * sine, second * cosine + first * sine], axis=-1
    )


def general(
    hidden_in, norm_gain, seq_lengths, w_query, b_query, w_key, b_key, w_value, b_value, w_out
):
    tok_rows = hidden_in.shape[0]
    gathered = lax.all_gather(hidden_in, "tp", axis=1, tiled=True)
    widened = gathered.astype(jnp.float32)
    normed = (
        widened * lax.rsqrt(jnp.mean(widened * widened, axis=-1, keepdims=True) + EPS) * norm_gain
    ).astype(jnp.bfloat16)
    cp_index = lax.axis_index("cp")
    positions = cp_index * tok_rows + jnp.arange(tok_rows, dtype=jnp.int32)
    docs, local_pos = doc_tables(seq_lengths, positions)
    query = jnp.dot(normed, w_query, preferred_element_type=jnp.float32) + b_query.astype(
        jnp.float32
    )
    query = rotate(query.reshape(tok_rows, -1, HD), local_pos).astype(jnp.bfloat16)
    key_heads = jnp.dot(normed, w_key, preferred_element_type=jnp.float32) + b_key.astype(
        jnp.float32
    )
    key_heads = rotate(key_heads.reshape(tok_rows, -1, HD), local_pos).astype(jnp.bfloat16)
    value_flat = (
        jnp.dot(normed, w_value, preferred_element_type=jnp.float32) + b_value.astype(jnp.float32)
    ).astype(jnp.bfloat16)
    kv_heads = key_heads.shape[1]
    value_heads = value_flat.reshape(tok_rows, kv_heads, HD)
    group = query.shape[1] // kv_heads
    grouped = query.reshape(tok_rows, kv_heads, group, HD)
    scale = HD ** (-0.5)

    def update(carried, key_block, value_block, start):
        count = key_block.shape[0]
        key_pos = start + jnp.arange(count, dtype=jnp.int32)
        key_docs, _ = doc_tables(seq_lengths, key_pos)
        allowed = (key_pos[None, :] <= positions[:, None]) & (key_docs[None, :] == docs[:, None])

        def compute(state):
            running, totals, accum = state
            scores = (
                jnp.einsum("qhgd,khd->hgqk", grouped, key_block, preferred_element_type=jnp.float32)
                * scale
            )
            highest = jnp.max(jnp.where(allowed, scores, NEG), axis=-1)
            fresh = jnp.maximum(running, highest)
            weights = jnp.where(allowed, jnp.exp(scores - fresh[..., None]), 0.0)
            factor = jnp.exp(running - fresh)
            totals = totals * factor + jnp.sum(weights, axis=-1)
            added = jnp.einsum(
                "hgqk,khd->qhgd",
                weights.astype(jnp.bfloat16),
                value_block,
                preferred_element_type=jnp.float32,
            )
            accum = accum * jnp.transpose(factor, (2, 0, 1))[..., None] + added
            return (fresh, totals, accum)

        return lax.cond(jnp.any(allowed), compute, lambda state: state, carried)

    carried = (
        jnp.full((kv_heads, group, tok_rows), NEG, jnp.float32),
        jnp.zeros((kv_heads, group, tok_rows), jnp.float32),
        jnp.zeros((tok_rows, kv_heads, group, HD), jnp.float32),
    )
    key_rows = lax.all_gather(key_heads, "cp", axis=0, tiled=True)
    count = key_rows.shape[0]
    width = math.gcd(512, count)
    blocks = count // width
    key_split = key_rows.reshape(blocks, width, kv_heads, HD)
    value_split = lax.all_gather(value_heads, "cp", axis=0, tiled=True).reshape(
        blocks, width, kv_heads, HD
    )

    def advance(state, items):
        return (update(state, items[0], items[1], items[2] * width), None)

    carried, _ = lax.scan(
        advance, carried, (key_split, value_split, jnp.arange(blocks, dtype=jnp.int32))
    )
    _, totals, accum = carried
    attended = (
        (accum / jnp.transpose(totals, (2, 0, 1))[..., None])
        .astype(jnp.bfloat16)
        .reshape(tok_rows, -1)
    )
    summed = jnp.dot(
        lax.all_gather(attended, "tp", axis=1, tiled=True),
        w_out,
        preferred_element_type=jnp.float32,
    )
    mixed = (hidden_in.astype(jnp.float32) + summed).astype(jnp.bfloat16)
    return (mixed, key_heads.reshape(tok_rows, -1), value_flat)


def turned(u, cosf, sinf):
    return u * cosf + pltpu.roll(u, HD // 2, 1) * sinf


def kv_kernel(s_ref, own_ref, got_ref, gain_ref, cos_ref, sin_ref, wk_ref, wv_ref, bk_ref, bv_ref,
              k_ref, v_ref, keep_ref, send_ref, normed_ref):
    tp = s_ref[0]
    half = own_ref.shape[1]
    j = pl.program_id(0)

    @pl.when(j == 0)
    def _():
        own = own_ref[...].astype(jnp.float32)
        got = got_ref[...].astype(jnp.float32)
        total = jnp.sum(own * own, axis=1, keepdims=True) + jnp.sum(got * got, axis=1, keepdims=True)
        factor = lax.rsqrt(total / (2 * half) + EPS)
        here = pl.ds(pl.multiple_of(tp * half, half), half)
        there = pl.ds(pl.multiple_of((1 - tp) * half, half), half)
        normed_ref[:, here] = (own * factor * gain_ref[:, here]).astype(jnp.bfloat16)
        normed_ref[:, there] = (got * factor * gain_ref[:, there]).astype(jnp.bfloat16)

    x = normed_ref[...]
    keys = jnp.dot(x, wk_ref[...], preferred_element_type=jnp.float32) + bk_ref[...]
    cosf, sinf = cos_ref[...], sin_ref[...]
    width = keys.shape[1]
    keys = jnp.concatenate(
        [turned(keys[:, i:i + HD], cosf, sinf) for i in range(0, width, HD)], axis=1
    ).astype(jnp.bfloat16)
    values = (jnp.dot(x, wv_ref[...], preferred_element_type=jnp.float32) + bv_ref[...]).astype(
        jnp.bfloat16
    )
    k_ref[...] = keys
    v_ref[...] = values

    @pl.when(j == 0)
    def _():
        keep_ref[:, :width] = keys
        keep_ref[:, width:] = values

    @pl.when(j == 1)
    def _():
        send_ref[:, :width] = keys
        send_ref[:, width:] = values


def project_kv(scalars, own, got, gain, cosf, sinf, wk, wv, bk, bv):
    rows, half = own.shape
    depth, cols = wk.shape
    width = cols // 2
    whole = lambda shape: pl.BlockSpec(shape, lambda j, s: (0, 0))
    side = lambda j, s: (0, lax.rem(j + s[1], 2))
    bf = jnp.bfloat16
    return pl.pallas_call(
        kv_kernel,
        out_shape=(
            jax.ShapeDtypeStruct((rows, cols), bf),
            jax.ShapeDtypeStruct((rows, cols), bf),
            jax.ShapeDtypeStruct((rows, cols), bf),
            jax.ShapeDtypeStruct((rows, cols), bf),
            jax.ShapeDtypeStruct((rows, depth), bf),
        ),
        grid_spec=pltpu.PrefetchScalarGridSpec(
            num_scalar_prefetch=1,
            grid=(2,),
            in_specs=[
                whole((rows, half)), whole((rows, half)), whole((1, depth)),
                whole((rows, HD)), whole((rows, HD)),
                pl.BlockSpec((depth, width), side), pl.BlockSpec((depth, width), side),
                pl.BlockSpec((1, width), side), pl.BlockSpec((1, width), side),
            ],
            out_specs=[
                pl.BlockSpec((rows, width), side), pl.BlockSpec((rows, width), side),
                whole((rows, cols)), whole((rows, cols)), whole((rows, depth)),
            ],
        ),
        cost_estimate=pl.CostEstimate(
            flops=4 * rows * depth * cols, transcendentals=0, bytes_accessed=4 * depth * cols
        ),
        name="project_kv",
    )(scalars, own, got, gain, cosf, sinf, wk, wv, bk, bv)


def q_kernel(steps, s_ref, *refs):
    x_refs = refs[:CHUNKS]
    cos_ref, sin_ref, w_ref, b_ref, keep_ref, send_ref, x_all = refs[CHUNKS:]
    j = pl.program_id(0)
    rows = x_refs[0].shape[0]

    @pl.when(j == 0)
    def _():
        for t, x_ref in enumerate(x_refs):
            x_all[t * rows:(t + 1) * rows, :] = x_ref[...]

    q = jnp.dot(x_all[...], w_ref[...], preferred_element_type=jnp.float32) + b_ref[...]
    cosf, sinf = cos_ref[...], sin_ref[...]
    q = jnp.concatenate(
        [turned(q[:, i:i + HD], cosf, sinf) for i in range(0, q.shape[1], HD)], axis=1
    ).astype(jnp.bfloat16)

    @pl.when(j < steps)
    def _():
        keep_ref[...] = q

    @pl.when(j >= steps)
    def _():
        send_ref[...] = q


def project_q(scalars, normed, cosf, sinf, wq, bq):
    rows, depth = normed[0].shape
    tokens = rows * len(normed)
    cols = wq.shape[1]
    width = math.gcd(cols // 2, 2 * HD)
    steps = cols // 2 // width
    whole = lambda shape: pl.BlockSpec(shape, lambda j, s: (0, 0))
    side = lambda j, s: (0, lax.rem(j // steps + s[1], 2) * steps + lax.rem(j, steps))
    return pl.pallas_call(
        functools.partial(q_kernel, steps),
        out_shape=(jax.ShapeDtypeStruct((tokens, cols // 2), jnp.bfloat16),) * 2,
        grid_spec=pltpu.PrefetchScalarGridSpec(
            num_scalar_prefetch=1,
            grid=(2 * steps,),
            in_specs=[whole((rows, depth))] * len(normed) + [
                whole((tokens, HD)), whole((tokens, HD)),
                pl.BlockSpec((depth, width), side), pl.BlockSpec((1, width), side),
            ],
            out_specs=[
                pl.BlockSpec((tokens, width), lambda j, s: (0, jnp.minimum(j, steps - 1))),
                pl.BlockSpec((tokens, width), lambda j, s: (0, jnp.maximum(j - steps, 0))),
            ],
            scratch_shapes=[pltpu.VMEM((tokens, depth), jnp.bfloat16)],
        ),
        cost_estimate=pl.CostEstimate(
            flops=2 * tokens * depth * cols, transcendentals=0, bytes_accessed=2 * depth * cols
        ),
        name="project_q",
    )(scalars, *normed, cosf, sinf, wq, bq)


def attend_kernel(units, heads, group, first, last, t_ref, *refs):
    q_refs, refs = refs[:2], refs[2:]
    pos_ref, low_ref, refs = refs[0], refs[1], refs[2:]
    u_refs, refs = refs[:units * CHUNKS], refs[units * CHUNKS:]
    if not first:
        (m_in, l_in, acc_in), refs = refs[:3], refs[3:]
    if last:
        out_refs, refs = refs[:2], refs[2:]
    m_ref, l_ref, acc_ref, kv, q_all = refs
    keys = u_refs[0].shape[0]
    part = keys // 2
    span = keys * CHUNKS
    many = heads * group
    tiles = 2 * many
    if first:
        m_ref[...] = jnp.full(m_ref.shape, NEG, jnp.float32)
        l_ref[...] = jnp.zeros(l_ref.shape, jnp.float32)
        acc_ref[...] = jnp.zeros(acc_ref.shape, jnp.float32)
    else:
        m_ref[...] = m_in[...]
        l_ref[...] = l_in[...]
        acc_ref[...] = acc_in[...]
    for n in range(units):
        for t in range(CHUNKS):
            kv[n, t * keys:(t + 1) * keys, :] = u_refs[n * CHUNKS + t][...]
    for half in range(2):
        for g in range(many):
            q_all[half * many + g] = q_refs[half][:, g * HD:(g + 1) * HD]
    factor = HD ** (-0.5) * math.log2(math.e)

    def step(n, masked):
        allowed = None
        if masked:
            at = lax.broadcasted_iota(jnp.int32, (span, 1), 0)
            chunk = at // keys
            inner = at - chunk * keys
            base = jnp.where(inner < part, t_ref[n, 1], t_ref[n, 2] - part)
            at = base + inner + chunk * part
            allowed = [(at >= low_ref[h]) & (at <= pos_ref[h]) for h in range(2)]

        def scores(i):
            head = i % many // group
            return lax.dot_general(
                kv[n, :, head * HD:(head + 1) * HD], q_all[i], (((1,), (1,)), ((), ())),
                preferred_element_type=jnp.float32,
            )

        def soften(i, s):
            if masked:
                s = jnp.where(allowed[i // many], s, NEG)
            old = m_ref[i]
            new = jnp.maximum(old, jnp.max(s, axis=0, keepdims=True))
            p = jnp.exp2((s - new) * factor)
            if masked:
                p = jnp.where(allowed[i // many], p, 0.0)
            alpha = jnp.exp2((old - new) * factor)
            m_ref[i] = new
            l_ref[i] = l_ref[i] * alpha + jnp.sum(p, axis=0, keepdims=True)
            return p.astype(jnp.bfloat16), alpha

        def gather(i, p, alpha):
            head = heads + i % many // group
            added = lax.dot_general(
                kv[n, :, head * HD:(head + 1) * HD], p, (((0,), (0,)), ((), ())),
                preferred_element_type=jnp.float32,
            )
            acc_ref[i] = acc_ref[i] * alpha + added

        made, soft = {}, {}
        for i in range(tiles + 2):
            if i < tiles:
                made[i] = scores(i)
            if i >= 2:
                gather(i - 2, *soft.pop(i - 2))
            if 0 <= i - 1 < tiles:
                soft[i - 1] = soften(i - 1, made.pop(i - 1))

    def unit(n, carry):
        state = t_ref[n, 0]

        @pl.when(state == 1)
        def _():
            step(n, False)

        @pl.when(state == 2)
        def _():
            step(n, True)

        return carry

    lax.fori_loop(0, units, unit, 0)
    if last:
        for half in range(2):
            for g in range(many):
                i = half * many + g
                done = acc_ref[i] * (1.0 / l_ref[i])
                out_refs[half][:, g * HD:(g + 1) * HD] = done.T.astype(jnp.bfloat16)


def attend(table, queries, pos, low, units, state, heads, group, last):
    rows, cols = queries[0].shape
    keys, width = units[0].shape
    count = len(units) // CHUNKS
    tiles = 2 * heads * group
    first = state is None
    vm = pl.BlockSpec(memory_space=pltpu.VMEM)
    stat = jax.ShapeDtypeStruct((tiles, 1, rows), jnp.float32)
    accs = jax.ShapeDtypeStruct((tiles, HD, rows), jnp.float32)
    scratch = [
        pltpu.VMEM((count, keys * CHUNKS, width), jnp.bfloat16),
        pltpu.VMEM((tiles, rows, HD), jnp.bfloat16),
    ]
    if last:
        out_shape = (jax.ShapeDtypeStruct((rows, cols), jnp.bfloat16),) * 2
        scratch = [
            pltpu.VMEM(stat.shape, jnp.float32), pltpu.VMEM(stat.shape, jnp.float32),
            pltpu.VMEM(accs.shape, jnp.float32),
        ] + scratch
    else:
        out_shape = (stat, stat, accs)
    args = [*queries, pos, low, *units] + ([] if first else list(state))
    return pl.pallas_call(
        functools.partial(attend_kernel, count, heads, group, first, last),
        out_shape=out_shape,
        in_specs=[pl.BlockSpec(memory_space=pltpu.SMEM)] + [vm] * len(args),
        out_specs=[vm] * len(out_shape),
        scratch_shapes=scratch,
        cost_estimate=pl.CostEstimate(
            flops=4 * tiles * rows * keys * HD * len(units),
            transcendentals=tiles * rows * keys * len(units),
            bytes_accessed=4 * tiles * rows * HD,
        ),
    )(table, *args)


def out_kernel(s_ref, h_ref, *refs):
    out_ref = refs[-1]
    count = (len(refs) - 1) // 2
    total = h_ref[...].astype(jnp.float32)
    for a_ref, w_ref in zip(refs[:count], refs[count:-1]):
        total = total + jnp.dot(a_ref[...], w_ref[...], preferred_element_type=jnp.float32)
    out_ref[...] = total.astype(out_ref.dtype)


def project_out(scalars, base, pieces, slabs, w_out, dtype):
    rows, cols = base.shape
    depth = pieces[0].shape[1]
    width = math.gcd(cols, 512)
    whole = lambda a: pl.BlockSpec(a.shape, lambda j, s: (0, 0))
    across = pl.BlockSpec((rows, width), lambda j, s: (0, j))
    return pl.pallas_call(
        out_kernel,
        out_shape=jax.ShapeDtypeStruct((rows, cols), dtype),
        grid_spec=pltpu.PrefetchScalarGridSpec(
            num_scalar_prefetch=1,
            grid=(cols // width,),
            in_specs=[across]
            + [whole(a) for a in pieces]
            + [pl.BlockSpec((depth, width), lambda j, s, n=n: (s[n], j)) for n in slabs],
            out_specs=across,
        ),
        cost_estimate=pl.CostEstimate(
            flops=2 * rows * depth * cols * len(pieces), transcendentals=0,
            bytes_accessed=2 * depth * cols * len(pieces),
        ),
    )(scalars, base, *pieces, *[w_out] * len(pieces))


def local(
    planes, hidden_in, norm_gain, seq_lengths, w_query, b_query, w_key, b_key, w_value, b_value,
    w_out,
):
    rows, _ = hidden_in.shape
    part = rows // CHUNKS
    heads = w_key.shape[1] // HD // 2
    group = w_query.shape[1] // w_key.shape[1]
    tp = lax.axis_index("tp")
    cp = lax.axis_index("cp")
    core, row, plane = cp % 2, cp // 2 % 2, cp // 4
    chip = cp // 2
    f32 = jnp.float32

    def pairs(move):
        found = []
        for z in range(planes):
            for y in range(2):
                for c in range(2):
                    for x in range(2):
                        to = move(z, y, c, x)
                        if to is not None:
                            found.append((
                                ((z * 2 + y) * 2 + c) * 2 + x,
                                ((to[0] * 2 + to[1]) * 2 + to[2]) * 2 + to[3],
                            ))
        return found

    over_x = pairs(lambda z, y, c, x: (z, y, c, 1 - x))
    over_c = pairs(lambda z, y, c, x: (z, y, 1 - c, x))
    over_xc = pairs(lambda z, y, c, x: (z, y, 1 - c, 1 - x))

    def up(k):
        return pairs(lambda z, y, c, x: (z + 1, y, c, x) if k <= z + 1 < planes else None)

    def across(k):
        return pairs(
            lambda z, y, c, x: (z, 1 - y, c, x) if z >= k and (k > 0 or y == 0) else None
        )

    def send(a, route):
        return lax.ppermute(a, SIZES, route)

    chunks = [hidden_in[t * part:(t + 1) * part] for t in range(CHUNKS)]
    got = [send(a, over_x) for a in chunks]

    ends = jnp.cumsum(seq_lengths)
    starts = ends - seq_lengths
    chip_pos = jnp.stack([
        cp * rows + jnp.arange(rows, dtype=jnp.int32),
        (cp + 1 - 2 * core) * rows + jnp.arange(rows, dtype=jnp.int32),
    ])
    low = jnp.max(
        jnp.where(starts[None, None, :] <= chip_pos[..., None], starts[None, None, :], 0), axis=-1
    )
    local_pos = (chip_pos - low)[0]
    freq = ROPE_BASE ** (-jnp.arange(HD // 2, dtype=f32) / (HD // 2))
    angle = local_pos.astype(f32)[:, None] * freq[None, :]
    cosine, sine = jnp.cos(angle), jnp.sin(angle)
    cosf = jnp.concatenate([cosine, cosine], axis=1)
    sinf = jnp.concatenate([-sine, sine], axis=1)
    other = (1 - tp) * 2
    scalars = jnp.stack(
        [tp, core, tp * 2 + core, tp * 2 + 1 - core, other + core, other + 1 - core]
    ).astype(jnp.int32)

    span = 2 * rows
    q_from, q_to = chip * span, chip * span + span - 1
    low_min = jnp.min(low)
    low_max = jnp.max(low)
    number = jnp.arange(2 * planes, dtype=jnp.int32)
    source = (plane - number // 2) * 2 + jnp.where(number % 2 == 0, row, 1 - row)
    first_pos = source * span + core * rows
    second_pos = source * span + (1 - core) * rows
    k_from = source * span
    k_to = k_from + span - 1
    valid = (source >= 0) & (k_to >= low_min) & (k_from <= q_to)
    free = (k_from >= low_max) & (k_to <= q_from)
    states = jnp.where(valid, jnp.where(free, 1, 2), 0)
    table = jnp.stack([states, first_pos, second_pos], axis=1).astype(jnp.int32)

    gain = norm_gain[None, :]
    bk, bv, bq = (b.astype(f32)[None, :] for b in (b_key, b_value, b_query))
    k_parts, v_parts, normed, units = [], [], [], [[None] * CHUNKS for _ in range(2 * planes)]
    for t in range(CHUNKS):
        here = slice(t * part, (t + 1) * part)
        k, v, keep, give, norm = project_kv(
            scalars, chunks[t], got[t], gain, cosf[here], sinf[here],
            w_key, w_value, bk, bv,
        )
        k_parts.append(k)
        v_parts.append(v)
        normed.append(norm)
        column = jnp.concatenate([keep, send(give, over_c)], axis=0)
        for k in range(planes):
            units[2 * k][t] = column
            units[2 * k + 1][t] = send(column, across(k))
            if k + 1 < planes:
                column = send(column, up(k + 1))
    q_keep, q_give = project_q(scalars, normed, cosf, sinf, w_query, bq)
    queries = (q_keep, send(q_give, over_c))

    pos, low = chip_pos[:, None, :], low[:, None, :]
    state = None
    for planes_here in ((0,), tuple(range(1, planes - 1)), (planes - 1,)):
        if not planes_here:
            continue
        mine, lines = [], []
        for k in planes_here:
            for flip in range(2):
                mine.extend(units[2 * k + flip])
                lines.append(2 * k + flip)
        state = attend(
            table[lines[0]:lines[-1] + 1], queries, pos, low, mine, state, heads, group,
            planes_here[-1] == planes - 1,
        )
    att_own, att_partner = state
    swapped = send(att_partner, over_c)
    crossed = send(att_own, over_x)
    diagonal = send(att_partner, over_xc)
    total = project_out(scalars, hidden_in, (att_own, swapped), (2, 3), w_out, f32)
    total = project_out(scalars, total, (crossed,), (4,), w_out, f32)
    mixed = project_out(scalars, total, (diagonal,), (5,), w_out, jnp.bfloat16)
    return (mixed, jnp.concatenate(k_parts, axis=0), jnp.concatenate(v_parts, axis=0))


def solution(mesh):
    placed = (
        P("cp", "tp"),
        P(),
        P(),
        P(None, "tp"),
        P("tp"),
        P(None, "tp"),
        P("tp"),
        P(None, "tp"),
        P("tp"),
        P(None, "tp"),
    )
    out = (P("cp", "tp"), P("cp", "tp"), P("cp", "tp"))

    def call(*args):
        cp, tp = mesh.shape["cp"], mesh.shape["tp"]
        rows = args[0].shape[0] // cp
        kv_heads = args[5].shape[1] // tp // HD
        fits = tp == 2 and cp % 4 == 0 and cp >= 12 and kv_heads % 2 == 0 and rows % 32 == 0
        if not fits:
            return jax.shard_map(
                general, mesh=mesh, in_specs=placed, out_specs=out, check_vma=False
            )(*args)

        def body(*args):
            return local(cp // 4, *args)

        step = jax.shard_map(body, mesh=mesh, in_specs=placed, out_specs=out, check_vma=False)
        return step(*args)

    return call
```
